256 devices in a mesh: dp: 4 (over y), tensor: 8 (over z), pipe: 8 (over x, core).
Axes of the slice: x: 4, y: 4, z: 8, core: 2. Of those that a mesh axis runs over, the one named last changes fastest.
Arguments:
- acts: bfloat16 [24576, 4096], P(('dp', 'pipe')), may hold values from -6 to 6
- grad_hidden: bfloat16 [24576, 14336], P(('dp', 'pipe'), 'tensor'), may hold values from -384 to 384
- token_count: int32 [32], P(('dp', 'pipe')), may hold values from 1 to 768, as said below
- hot_ids: int32 [8, 179], P('tensor'), may hold values from 0 to 1791, as said below
- block_owner: int32 [112, 1], P('tensor'), may hold values from 0 to 7; in each aligned block of 14 rows (0 to 13, 14 to 27, ...) at most 4 rows name the same one
- master_hot: float32 [1432, 4096], P('tensor', ('dp', 'pipe')), may hold values from -6 to 6
- moment_hot: float32 [1432, 4096], P('tensor', ('dp', 'pipe')), may hold values from -3 to 3
- second_hot: float32 [1432, 4096], P('tensor', ('dp', 'pipe')), may hold values from 0.1 to 100
Outputs:
- new_master: float32 [1432, 4096], P('tensor', ('dp', 'pipe'))
- new_moment: float32 [1432, 4096], P('tensor', ('dp', 'pipe'))
- new_second: float32 [1432, 4096], P('tensor', ('dp', 'pipe'))
- hot_weights: bfloat16 [1432, 4096], P('tensor', 'dp')
- cold_sectioning: bfloat16 [256, 4096, 128], P('tensor', ('dp', 'pipe'))
The draws below stay inside these ranges and needn't reach their ends.
Inputs may be any that keep to these rules, and one draw needn't show every extreme that they name: `token_count`: each micro-batch has at least one live token, and some micro-batch has exactly 768. `hot_ids`: each row lists 179 different offsets. `block_owner`: within the 14 blocks of one tensor index, no owner is named more than 4 times.
All inputs are finite; a program needn't handle non-finite values.
Results may differ from the reference program's by a relative error of at most 0.015.
Values may be sent and summed in bfloat16 or wider, within the bound.
No kernel may reach another device: no remote copies, remote signals or barrier semaphores. Data moves between devices by JAX's collectives and lax.ppermute only.
A program may use at most 128 MiB of HBM per device.

```python
import math
import jax
import jax.numpy as jnp
import numpy as np
from jax import lax

D = 4096
FF = 14336
TOK_DEV = 768
CB = 128
GROUPS = 32
TOKENS = 24576
FFS = 1792
HOT_TP = 179
HOT = 1432
BLOCKS = 14
SLOTS = 4
N_TENSOR = 8


def draw_token_count(key, part):
    index = jnp.arange(GROUPS, dtype=jnp.int32)
    low = TOK_DEV // 4
    base = low + (TOK_DEV - low) * index // max(GROUPS - 1, 1)
    jitter = jax.random.randint(jax.random.fold_in(key, 5), (GROUPS,), 0, max(TOK_DEV // 8, 1) + 1)
    jitter = jnp.where(index == GROUPS - 1, 0, jitter)
    return jnp.maximum(base - jitter, 1).astype(jnp.int32)


def draw_hot_ids(key, part):
    keys = jax.random.split(jax.random.fold_in(key, 17), N_TENSOR)

    def choose(single):
        return jax.random.permutation(single, FFS)[:HOT_TP]
    return jax.vmap(choose)(keys).astype(jnp.int32)


def block_levels(key, extent, cuts, smallest, top_value):
    def one(axis_at, blocks):
        heights = jax.random.uniform(jax.random.fold_in(jax.random.fold_in(key, 6), axis_at), (blocks,), jnp.float32, smallest / len(cuts), top_value / len(cuts))
        return jnp.repeat(jnp.exp(heights), extent[axis_at] // blocks).reshape((-1,) + (1,) * (len(extent) - axis_at - 1))

    loudness = one(*cuts[0])
    for cut in cuts[1:]:
        loudness = loudness * one(*cut)
    return loudness


def routed_block(own_key, own, number, rows, amount, top, most, slope):
    sequence = jax.random.permutation(own_key, amount)
    heavy_load, usual = load_shares(amount, rows * top, most, slope, True), load_shares(amount, rows * top, most, slope, False)
    places = jnp.arange(amount)

    def named(sizes, offset_by):
        used = int((sizes > 0).sum())
        fixed = max(1, used // 4)
        passed = fixed + (places - fixed + offset_by * (used - fixed)) % max(1, amount - fixed)
        return jnp.zeros((amount,), jnp.int32).at[sequence[jnp.where(places < fixed, places, passed)]].set(jnp.asarray(sizes, jnp.int32))

    sizes = jnp.where(number % 4 == 0, named(heavy_load, number // 4), named(usual, number - number // 4 - 1))
    mixed = jax.random.permutation(jax.random.fold_in(own, 3), amount)
    donor, receiver = mixed[0:amount // 2 * 2:2], mixed[1:amount // 2 * 2:2]
    room = jnp.minimum(sizes[donor] - 1, most - sizes[receiver]) // 2
    room = jnp.where((donor == sequence[0]) | (receiver == sequence[0]) | (sizes[receiver] == 0), 0, jnp.maximum(room, 0))
    passed = jax.random.randint(jax.random.fold_in(own, 4), (amount // 2,), 0, 1 << 20) % (room + 1)
    sizes = sizes.at[donor].add(-passed).at[receiver].add(passed)
    members = jnp.searchsorted(jnp.cumsum(sizes), jnp.arange(rows * top), side="right").astype(jnp.int32)
    listing = members.reshape(top, rows).T
    listing = listing[jax.random.permutation(jax.random.fold_in(own, 1), rows)]
    offset_by = jax.random.randint(jax.random.fold_in(own, 2), (rows, 1), 0, top)
    return jnp.take_along_axis(listing, (jnp.arange(top)[None, :] + offset_by) % top, axis=1)


def load_shares(count, total, reach, lean, full):
    loads = [(1 << 20) // math.isqrt(standing ** lean) + 1 for standing in range(1, count + 1)]
    largest = reach if full else min(reach, max(-(-total // count), total * loads[0] // sum(loads)))
    least = 1 if total - largest >= count - 1 else 0
    counts, rest = [largest] + [least] * (count - 1), total - largest - least * (count - 1)
    while rest > 0:
        candidates = [i for i in range(1, count) if counts[i] < largest] or [i for i in range(1, count) if counts[i] < reach]
        whole, budget = sum([loads[i] for i in candidates]), rest
        for i in candidates:
            extra = min(reach - counts[i], max(1, budget * loads[i] // whole), rest)
            counts[i] = counts[i] + extra
            rest = rest - extra
    return np.array(counts)


def normal_values(own_key, shape, spread, limit, cuts=(), kind=jnp.bfloat16):
    values = spread * jax.random.normal(own_key, shape, jnp.float32)
    if cuts:
        values = values * block_levels(own_key, shape, cuts, -0.22, 0.18)
    return jnp.clip(values, -limit, limit).astype(kind)


def setup_inputs(seed: int = 0) -> dict:
    key_list = jax.random.split(jax.random.key(seed), 9)
    acts = normal_values(key_list[0], (TOKENS, D), 1.0, 6.0, ((0, 32),))
    grad_hidden = normal_values(key_list[1], (TOKENS, FF), 64.0, 384.0, ((0, 32), (1, 8)))
    token_count = draw_token_count(jax.random.fold_in(key_list[8], 71), 0)
    hot_ids = draw_hot_ids(jax.random.fold_in(key_list[8], 71), 0)
    block_owner_keys = jax.random.split(jax.random.fold_in(key_list[4], 1), (N_TENSOR * BLOCKS) // BLOCKS)
    block_owner_turns = jax.random.permutation(jax.random.fold_in(key_list[4], 3), (N_TENSOR * BLOCKS) // BLOCKS)
    block_owner = jax.vmap(lambda own, number: routed_block(jax.random.fold_in(key_list[4], 2), own, number, BLOCKS, N_TENSOR, 1, SLOTS, 2))(block_owner_keys, block_owner_turns).reshape((N_TENSOR * BLOCKS, 1))
    master_hot = normal_values(key_list[5], (HOT, D), 1.0, 6.0, ((0, 8), (1, 32)), jnp.float32)
    moment_hot = normal_values(key_list[6], (HOT, D), 0.5, 3.0, ((0, 8), (1, 32)), jnp.float32)
    second_hot = jnp.clip(jnp.exp(math.log(100.0) - 6.9077553 * jax.random.uniform(key_list[7], (HOT, D), jnp.float32) ** block_levels(key_list[7], (HOT, D), ((0, 8), (1, 32)), -0.2, 0.2)), 0.1, 100.0)
    return {"acts": acts, "grad_hidden": grad_hidden, "token_count": token_count, "hot_ids": hot_ids, "block_owner": block_owner, "master_hot": master_hot, "moment_hot": moment_hot, "second_hot": second_hot}


def reference(acts, grad_hidden, token_count, hot_ids, block_owner, master_hot, moment_hot, second_hot):
    slot_pos = jnp.arange(TOKENS, dtype=jnp.int32) % TOK_DEV
    live = slot_pos < jnp.repeat(token_count, TOK_DEV)
    masked = jnp.where(live[:, None], grad_hidden, jnp.zeros_like(grad_hidden))
    total = jnp.sum(token_count.astype(jnp.float32))
    inputs = acts.reshape(GROUPS, TOK_DEV, D)
    outputs = masked.reshape(GROUPS, TOK_DEV, FF)

    def accumulate(carry, pair):
        left, right = pair
        partial_value = jnp.dot(left.T, right, preferred_element_type=jnp.float32).astype(jnp.bfloat16)
        partial_value = lax.optimization_barrier(partial_value)
        return (carry + partial_value.astype(jnp.float32), None)
    summed, _ = lax.scan(accumulate, jnp.zeros((D, FF), jnp.float32), (inputs, outputs))
    grad = summed / total
    hot_cols = (jnp.arange(N_TENSOR, dtype=jnp.int32)[:, None] * FFS + hot_ids).reshape(HOT).astype(jnp.int32)
    g_hot = grad[:, hot_cols].T
    new_moment = 0.9 * moment_hot + 0.1 * g_hot
    new_second = 0.95 * second_hot + 0.05 * g_hot * g_hot
    bias_one = 1.0 - 0.9 ** 4
    bias_two = 1.0 - 0.95 ** 4
    new_master = master_hot - 0.02 * (new_moment / bias_one) / (jnp.sqrt(new_second / bias_two) + 1e-08)
    hot_weights = new_master.astype(jnp.bfloat16)
    is_hot = jnp.zeros((FF,), jnp.bool_).at[hot_cols].set(True)
    cold = jnp.where(is_hot[None, :], 0.0, grad).astype(jnp.bfloat16)
    blocks = cold.reshape(D, N_TENSOR, BLOCKS, CB).transpose(1, 2, 0, 3)
    owner = block_owner.reshape(N_TENSOR, BLOCKS)
    same = owner[:, :, None] == owner[:, None, :]
    index = jnp.arange(BLOCKS, dtype=jnp.int32)
    earlier = index[None, :] < index[:, None]
    slot = lax.optimization_barrier(jnp.sum((same & earlier[None, :, :]).astype(jnp.int32), axis=2))
    source = jnp.arange(N_TENSOR, dtype=jnp.int32)[:, None]
    target = ((owner * N_TENSOR + source) * SLOTS + slot).reshape(-1).astype(jnp.int32)
    sectioning = jnp.zeros((N_TENSOR * N_TENSOR * SLOTS, D, CB), jnp.bfloat16)
    cold_sectioning = sectioning.at[target].set(blocks.reshape(N_TENSOR * BLOCKS, D, CB))
    return (new_master, new_moment, new_second, hot_weights, cold_sectioning)
```

```python
import functools

import jax
import jax.numpy as jnp
import numpy as np
from jax import lax
from jax.experimental import pallas as pl
from jax.experimental.pallas import tpu as pltpu
from jax.sharding import Mesh
from jax.sharding import PartitionSpec as P


CB = 128
DP_PIPE = ("dp", "pipe_0", "pipe_1")
SLOTS = 4
COLOURS = ((0, 4), (4, 4), (8, 3), (11, 3))
SPARE = 16
EVEN = [(0, 1), (1, 0), (2, 3), (3, 2)]
ODD = [(1, 2), (2, 1), (3, 0), (0, 3)]
DIMS = (("pipe_0", EVEN), ("dp", EVEN), ("pipe_0", ODD), ("dp", ODD))
SWAP = [(0, 1), (1, 0)]
MiB = 1 << 20


def gray(p):
    return p ^ (p >> 1)


def relative_table():
    rx = np.zeros((4, 2, 2, 8), np.int32)
    ry = np.zeros((4, 2, 2, 8), np.int32)
    rc = np.zeros((4, 2, 2, 8), np.int32)
    for k in range(4):
        for half in range(2):
            for own in range(2):
                for q in range(8):
                    idx = half * 8 + q
                    for s in range(4):
                        bit = (idx >> (3 - s)) & 1
                        d = (k + s) % 4
                        if d % 2 == 0:
                            rx[k, half, own, q] |= bit << (d // 2)
                        else:
                            ry[k, half, own, q] |= bit << (d // 2)
                    rc[k, half, own, q] = 1 - own
    return rx.reshape(-1), ry.reshape(-1), rc.reshape(-1)


def table_offset(k, half, own):
    return ((k * 2 + half) * 2 + own) * 8


def load_kernel(cnt_ref, a_hbm, g_hbm, a_ref, l0, l1, l2, l3, stage, a_sem, g_sem):
    toks = stage.shape[1]
    g_copies = [
        pltpu.make_async_copy(
            g_hbm.at[:, first * CB : (first + n) * CB],
            stage.at[k, :, : n * CB],
            g_sem.at[k],
        )
        for k, (first, n) in enumerate(COLOURS)
    ]
    a_copy = pltpu.make_async_copy(a_hbm, a_ref, a_sem)
    for cp in g_copies:
        cp.start()
    a_copy.start()
    live = lax.broadcasted_iota(jnp.int32, (toks, CB), 0) < cnt_ref[0]
    for k, ((first, n), out) in enumerate(zip(COLOURS, (l0, l1, l2, l3))):
        g_copies[k].wait()
        for i in range(n):
            v = stage[k, :, i * CB : (i + 1) * CB]
            out[i * CB : (i + 1) * CB, :] = jnp.where(live, v, jnp.zeros_like(v)).T
    a_copy.wait()


VM = pl.BlockSpec(memory_space=pltpu.VMEM)
HB = pl.BlockSpec(memory_space=pl.ANY)


def loaded(cnt, acts, grad_hidden):
    toks = acts.shape[0]
    outs = [jax.ShapeDtypeStruct(acts.shape, acts.dtype)]
    outs += [jax.ShapeDtypeStruct((n * CB, toks), jnp.bfloat16) for _, n in COLOURS]
    return pl.pallas_call(
        load_kernel,
        grid_spec=pltpu.PrefetchScalarGridSpec(
            num_scalar_prefetch=1,
            grid=(),
            in_specs=[HB, HB],
            out_specs=[VM] * 5,
            scratch_shapes=[
                pltpu.VMEM((4, toks, 4 * CB), jnp.bfloat16),
                pltpu.SemaphoreType.DMA,
                pltpu.SemaphoreType.DMA((4,)),
            ],
        ),
        out_shape=outs,
        compiler_params=pltpu.CompilerParams(vmem_limit_bytes=16 * MiB),
        cost_estimate=pl.CostEstimate(flops=2000000000, bytes_accessed=0, transcendentals=0),
        name="load",
    )(cnt, acts, grad_hidden)


def mm_kernel(tbl_ref, cnt_ref, l_ref, a_ref, *outs, spare, offs):
    n = l_ref.shape[0]
    left = l_ref[...]
    for o_ref, off in zip(outs, offs):
        for i in range(4):
            blk = [
                a_ref[:, pl.ds(pl.multiple_of(tbl_ref[off + 2 * i + j] * CB, CB), CB)]
                for j in range(2)
            ]
            r = jnp.dot(
                left, jnp.concatenate(blk, axis=1), preferred_element_type=jnp.float32
            ).astype(jnp.bfloat16)
            o_ref[2 * i, :n, :] = r[:, :CB]
            o_ref[2 * i + 1, :n, :] = r[:, CB:]
        if spare:
            c = cnt_ref[0]
            row = lax.broadcasted_iota(jnp.int32, (SPARE, CB), 0)
            digit = jnp.where(
                row == 0, c & 7, jnp.where(row == 1, (c >> 3) & 7, jnp.where(row == 2, c >> 6, 0))
            )
            digit = digit.astype(jnp.float32).astype(jnp.bfloat16)
            for i in range(8):
                o_ref[i, n:, :] = digit


def product(tbl, cnt, left, acts, k, half, owns):
    toks = acts.shape[0]
    n = left.shape[0]
    spare = SPARE if k == 3 else 0
    offs = [table_offset(k, half, own) for own in owns]
    return pl.pallas_call(
        functools.partial(mm_kernel, spare=spare, offs=offs),
        grid_spec=pltpu.PrefetchScalarGridSpec(
            num_scalar_prefetch=2,
            grid=(),
            in_specs=[VM, VM],
            out_specs=[VM] * len(owns),
        ),
        out_shape=[jax.ShapeDtypeStruct((8, n + spare, CB), jnp.bfloat16)] * len(owns),
        compiler_params=pltpu.CompilerParams(vmem_limit_bytes=8 * MiB),
        cost_estimate=pl.CostEstimate(
            flops=2 * 8 * CB * n * toks * len(owns), bytes_accessed=0, transcendentals=0
        ),
        name="mm",
    )(tbl, cnt, left, acts)


def tail_kernel(
    ids_ref, tgt_ref, g0, g1, g2, g3, ma_ref, mo_ref, se_ref, *refs
):
    nma_ref, nmo_ref, nse_ref, hw_ref = refs[:4]
    z_refs = refs[4:12]
    acc, hot, pack = refs[12:]
    for (first, nblk), g in zip(COLOURS, (g0, g1, g2, g3)):
        acc[first * CB : (first + nblk) * CB, :] = g[: nblk * CB, :]
    digits = g3[COLOURS[3][1] * CB : COLOURS[3][1] * CB + 8, :]
    total = digits[0:1, :] + 8.0 * digits[1:2, :] + 64.0 * digits[2:3, :]
    pack[...] = jnp.zeros_like(pack)
    count = hot.shape[0]

    def take(i, _):
        h = ids_ref[i]
        hot[pl.ds(i, 1), :] = acc[pl.ds(h, 1), :]
        acc[pl.ds(h, 1), :] = jnp.zeros((1, CB), jnp.float32)
        return 0

    lax.fori_loop(0, count, take, 0, unroll=4)
    g_hot = hot[...] / total
    mo = 0.9 * mo_ref[...] + 0.1 * g_hot
    se = 0.95 * se_ref[...] + 0.05 * g_hot * g_hot
    bias_one = 1.0 - 0.9**4
    bias_two = 1.0 - 0.95**4
    ma = ma_ref[...] - 0.02 * (mo / bias_one) / (jnp.sqrt(se / bias_two) + 1e-08)
    nmo_ref[...] = mo
    nse_ref[...] = se
    nma_ref[...] = ma
    hw_ref[...] = ma.astype(jnp.bfloat16)
    for b in range(acc.shape[0] // CB):
        x = acc[b * CB : (b + 1) * CB, :] / total
        pack[tgt_ref[b]] = x.T.astype(jnp.bfloat16)
    for d in range(8):
        z_refs[d][...] = pack[d * SLOTS : (d + 1) * SLOTS]


def tail(ids, tgt, gs, master, moment, second):
    hot = master.shape[0]
    f32 = jax.ShapeDtypeStruct(master.shape, jnp.float32)
    outs = [f32, f32, f32, jax.ShapeDtypeStruct(master.shape, jnp.bfloat16)]
    outs += [jax.ShapeDtypeStruct((SLOTS, CB, CB), jnp.bfloat16)] * 8
    vm = pl.BlockSpec(memory_space=pltpu.VMEM)
    return pl.pallas_call(
        tail_kernel,
        grid_spec=pltpu.PrefetchScalarGridSpec(
            num_scalar_prefetch=2,
            grid=(),
            in_specs=[vm] * 7,
            out_specs=[vm] * 12,
            scratch_shapes=[
                pltpu.VMEM((14 * CB, CB), jnp.float32),
                pltpu.VMEM((hot, CB), jnp.float32),
                pltpu.VMEM((8 * SLOTS, CB, CB), jnp.bfloat16),
            ],
        ),
        out_shape=outs,
        compiler_params=pltpu.CompilerParams(vmem_limit_bytes=24 * MiB),
        name="tail",
    )(ids, tgt, *gs, master, moment, second)


def join_kernel(pos_ref, a_ref, b_ref, c_ref, d_ref, o_ref):
    for r, piece in enumerate(
        (a_ref[...], b_ref[...], c_ref[0], c_ref[1], d_ref[0], d_ref[1], d_ref[2], d_ref[3])
    ):
        o_ref[:, pl.ds(pl.multiple_of(pos_ref[r] * CB, CB), CB)] = piece


def joined(pos, a, b, c, d):
    vm = pl.BlockSpec(memory_space=pltpu.VMEM)
    return pl.pallas_call(
        join_kernel,
        grid_spec=pltpu.PrefetchScalarGridSpec(
            num_scalar_prefetch=1, grid=(), in_specs=[vm] * 4, out_specs=vm
        ),
        out_shape=jax.ShapeDtypeStruct((a.shape[0], 8 * CB), a.dtype),
        compiler_params=pltpu.CompilerParams(vmem_limit_bytes=8 * MiB),
        name="join",
    )(pos, a, b, c, d)


def wide(*xs):
    out = xs[0].astype(jnp.float32)
    for x in xs[1:]:
        out = out + x.astype(jnp.float32)
    return out


def shards(
    acts, grad_hidden, token_count, hot_ids, block_owner, master_hot, moment_hot, second_hot
):
    y = lax.axis_index("dp")
    x = lax.axis_index("pipe_0")
    c = lax.axis_index("pipe_1")
    z = lax.axis_index("tensor")
    rx, ry, rc = relative_table()
    tbl = gray(gray(y) ^ ry) * 8 + gray(gray(x) ^ rx) * 2 + (c ^ rc)
    tbl = tbl.astype(jnp.int32)
    blocks = block_owner.shape[0]
    owner = block_owner[:, 0]
    same = owner[:, None] == owner[None, :]
    index = lax.broadcasted_iota(jnp.int32, (blocks, blocks), 0)
    other = lax.broadcasted_iota(jnp.int32, (blocks, blocks), 1)
    slot = jnp.sum((same & (other < index)).astype(jnp.int32), axis=1)
    tgt = ((owner - z) & 7) * SLOTS + slot

    acts_v, *left = loaded(token_count, acts, grad_hidden)

    def mm(k, half, owns):
        return product(tbl, token_count, left[k], acts_v, k, half, owns)

    def moved(v, axis, pairs):
        return lax.ppermute(v, axis, pairs)

    def summed(*xs):
        return wide(*xs).astype(jnp.bfloat16)

    first = []
    for k in range(4):
        (peer,) = mm(k, 1, (0,))
        got = moved(peer, "pipe_1", SWAP)
        (mine,) = mm(k, 1, (1,))
        first.append(moved(summed(mine, got), *DIMS[k]))
    parts = []
    for k in range(4):
        peer, mine = mm(k, 0, (0, 1))
        parts.append([mine, moved(peer, "pipe_1", SWAP), first[k]])
    size = 8
    for s in range(1, 4):
        half = size // 2
        for k in range(4):
            send = summed(*[p[half:size] for p in parts[k]])
            parts[k].append(moved(send, *DIMS[(k + s) % 4]))
        size = half
    gs = []
    for k in range(4):
        gs.append(wide(*[p[0] for p in parts[k]]))
    outs = tail(hot_ids[0], tgt, gs, master_hot, moment_hot, second_hot)
    new_master, new_moment, new_second, hw = outs[:4]
    packs = outs[4:]
    recv = [packs[0]]
    for d in range(1, 8):
        recv.append(moved(packs[d], "tensor", [(i, (i + d) % 8) for i in range(8)]))
    cold = jnp.zeros((8 * SLOTS, CB, CB), jnp.bfloat16)
    for d in range(8):
        cold = lax.dynamic_update_slice(cold, recv[d], (((z - d) & 7) * SLOTS, 0, 0))
    hw_b = moved(hw, "pipe_1", SWAP)
    two = jnp.stack([hw, hw_b])
    hw_c = moved(two, "pipe_0", EVEN)
    hw_d = moved(jnp.concatenate([two, hw_c]), "pipe_0", ODD)
    gx = np.array([0, 0, 1, 1, 2, 2, 3, 3], np.int32)
    cx = np.array([0, 1, 0, 1, 0, 1, 0, 1], np.int32)
    pos = (gray(gray(x) ^ gx) * 2 + (c ^ cx)).astype(jnp.int32)
    hot_weights = joined(pos, hw, hw_b, hw_c, hw_d)
    return (new_master, new_moment, new_second, hot_weights, cold)


def solution(mesh):
    split = Mesh(
        mesh.devices.reshape(mesh.shape["dp"], mesh.shape["tensor"], 4, 2),
        ("dp", "tensor", "pipe_0", "pipe_1"),
    )
    return jax.shard_map(
        shards,
        mesh=split,
        in_specs=(
            P(DP_PIPE, None),
            P(DP_PIPE, "tensor"),
            P(DP_PIPE),
            P("tensor", None),
            P("tensor", None),
            P("tensor", DP_PIPE),
            P("tensor", DP_PIPE),
            P("tensor", DP_PIPE),
        ),
        out_specs=(
            P("tensor", DP_PIPE),
            P("tensor", DP_PIPE),
            P("tensor", DP_PIPE),
            P("tensor", "dp"),
            P("tensor", DP_PIPE, None),
        ),
        check_vma=False,
    )
```

```python
import functools

import jax
import jax.numpy as jnp
from jax import lax
from jax.experimental import pallas as pl
from jax.experimental.pallas import tpu as pltpu
from jax.sharding import Mesh
from jax.sharding import PartitionSpec as P


CB = 128
DP_PIPE = ("dp", "pipe_0", "pipe_1")
SLOTS = 4
COLOURS = ((0, 4), (4, 4), (8, 3), (11, 3))
SPARE = 16
EVEN = [(0, 1), (1, 0), (2, 3), (3, 2)]
ODD = [(1, 2), (2, 1), (3, 0), (0, 3)]
DIMS = (("pipe_0", EVEN), ("dp", EVEN), ("pipe_0", ODD), ("dp", ODD))
SWAP = [(0, 1), (1, 0)]
MiB = 1 << 20


def gray(p):
    return p ^ (p >> 1)


def dest_block(k, half, own, q):
    idx = half * 8 + q
    rx = ry = 0
    for s in range(4):
        bit = (idx >> (3 - s)) & 1
        d = (k + s) % 4
        if d % 2 == 0:
            rx |= bit << (d // 2)
        else:
            ry |= bit << (d // 2)
    return far(lax.axis_index("dp"), ry) * 8 + pipe_block(rx, 1 - own)


def far(p, r):
    return gray(gray(p) ^ r)


def pipe_block(rx, rc):
    return far(lax.axis_index("pipe_0"), rx) * 2 + (lax.axis_index("pipe_1") ^ rc)


def load_kernel(cnt_ref, a_hbm, g_hbm, a_ref, l0, l1, l2, l3, stage, a_sem, g_sem):
    toks = stage.shape[1]
    g_copies = [
        pltpu.make_async_copy(
            g_hbm.at[:, first * CB : (first + n) * CB],
            stage.at[k, :, : n * CB],
            g_sem.at[k],
        )
        for k, (first, n) in enumerate(COLOURS)
    ]
    a_copy = pltpu.make_async_copy(a_hbm, a_ref, a_sem)
    for cp in g_copies:
        cp.start()
    a_copy.start()
    live = lax.broadcasted_iota(jnp.int32, (toks, CB), 0) < cnt_ref[0]
    for k, ((first, n), out) in enumerate(zip(COLOURS, (l0, l1, l2, l3))):
        g_copies[k].wait()
        for i in range(n):
            v = stage[k, :, i * CB : (i + 1) * CB]
            out[i * CB : (i + 1) * CB, :] = jnp.where(live, v, jnp.zeros_like(v)).T
    a_copy.wait()


VM = pl.BlockSpec(memory_space=pltpu.VMEM)
HB = pl.BlockSpec(memory_space=pltpu.HBM)


def loaded(cnt, acts, grad_hidden):
    toks = acts.shape[0]
    outs = [jax.ShapeDtypeStruct(acts.shape, acts.dtype)]
    outs += [jax.ShapeDtypeStruct((n * CB, toks), jnp.bfloat16) for _, n in COLOURS]
    return pl.pallas_call(
        load_kernel,
        grid_spec=pltpu.PrefetchScalarGridSpec(
            num_scalar_prefetch=1,
            grid=(),
            in_specs=[HB, HB],
            out_specs=[VM] * 5,
            scratch_shapes=[
                pltpu.VMEM((4, toks, 4 * CB), jnp.bfloat16),
                pltpu.SemaphoreType.DMA,
                pltpu.SemaphoreType.DMA((4,)),
            ],
        ),
        out_shape=outs,
        compiler_params=pltpu.CompilerParams(vmem_limit_bytes=16 * MiB),
        cost_estimate=pl.CostEstimate(flops=2000000000, bytes_accessed=0, transcendentals=0),
        name="load",
    )(
        cnt,
        pltpu.with_memory_space_constraint(acts, pltpu.HBM),
        pltpu.with_memory_space_constraint(grad_hidden, pltpu.HBM),
    )


def mm_kernel(cnt_ref, l_ref, a_ref, *outs, spare, k, half, owns):
    n = l_ref.shape[0]
    left = l_ref[...]
    for o_ref, own in zip(outs, owns):
        for i in range(4):
            blk = [
                a_ref[:, pl.ds(pl.multiple_of(dest_block(k, half, own, 2 * i + j) * CB, CB), CB)]
                for j in range(2)
            ]
            r = jnp.dot(
                left, jnp.concatenate(blk, axis=1), preferred_element_type=jnp.float32
            ).astype(jnp.bfloat16)
            o_ref[2 * i, :n, :] = r[:, :CB]
            o_ref[2 * i + 1, :n, :] = r[:, CB:]
        if spare:
            c = cnt_ref[0]
            row = lax.broadcasted_iota(jnp.int32, (SPARE, CB), 0)
            digit = jnp.where(
                row == 0, c & 7, jnp.where(row == 1, (c >> 3) & 7, jnp.where(row == 2, c >> 6, 0))
            )
            digit = digit.astype(jnp.float32).astype(jnp.bfloat16)
            for i in range(8):
                o_ref[i, n:, :] = digit


def product(cnt, left, acts, k, half, owns):
    toks = acts.shape[0]
    n = left.shape[0]
    spare = SPARE if k == 3 else 0
    return pl.pallas_call(
        functools.partial(mm_kernel, spare=spare, k=k, half=half, owns=owns),
        grid_spec=pltpu.PrefetchScalarGridSpec(
            num_scalar_prefetch=1,
            grid=(),
            in_specs=[VM, VM],
            out_specs=[VM] * len(owns),
        ),
        out_shape=[jax.ShapeDtypeStruct((8, n + spare, CB), jnp.bfloat16)] * len(owns),
        compiler_params=pltpu.CompilerParams(vmem_limit_bytes=8 * MiB),
        cost_estimate=pl.CostEstimate(
            flops=2 * 8 * CB * n * toks * len(owns), bytes_accessed=0, transcendentals=0
        ),
        name="mm",
    )(cnt, left, acts)


def tail_kernel(
    ids_ref, own_ref, g0, g1, g2, g3, ma_ref, mo_ref, se_ref, *refs
):
    nma_ref, nmo_ref, nse_ref, hw_ref = refs[:4]
    z_refs = refs[4:12]
    acc, hot, pack = refs[12:]
    for (first, nblk), g in zip(COLOURS, (g0, g1, g2, g3)):
        acc[first * CB : (first + nblk) * CB, :] = g[: nblk * CB, :]
    digits = g3[COLOURS[3][1] * CB : COLOURS[3][1] * CB + 8, :]
    total = digits[0:1, :] + 8.0 * digits[1:2, :] + 64.0 * digits[2:3, :]
    pack[...] = jnp.zeros_like(pack)
    count = hot.shape[0]

    def take(i, _):
        h = ids_ref[0, i]
        hot[pl.ds(i, 1), :] = acc[pl.ds(h, 1), :]
        acc[pl.ds(h, 1), :] = jnp.zeros((1, CB), jnp.float32)
        return 0

    lax.fori_loop(0, count, take, 0, unroll=4)
    g_hot = hot[...] / total
    mo = 0.9 * mo_ref[...] + 0.1 * g_hot
    se = 0.95 * se_ref[...] + 0.05 * g_hot * g_hot
    bias_one = 1.0 - 0.9**4
    bias_two = 1.0 - 0.95**4
    ma = ma_ref[...] - 0.02 * (mo / bias_one) / (jnp.sqrt(se / bias_two) + 1e-08)
    nmo_ref[...] = mo
    nse_ref[...] = se
    nma_ref[...] = ma
    hw_ref[...] = ma.astype(jnp.bfloat16)
    for b in range(acc.shape[0] // CB):
        x = acc[b * CB : (b + 1) * CB, :] / total
        owner = own_ref[b]
        slot = jnp.int32(0)
        for e in range(b):
            slot += (own_ref[e] == owner).astype(jnp.int32)
        pack[((owner - lax.axis_index("tensor")) & 7) * SLOTS + slot] = x.T.astype(jnp.bfloat16)
    for d in range(8):
        z_refs[d][...] = pack[d * SLOTS : (d + 1) * SLOTS]


def tail(ids, owners, gs, master, moment, second):
    hot = master.shape[0]
    f32 = jax.ShapeDtypeStruct(master.shape, jnp.float32)
    outs = [f32, f32, f32, jax.ShapeDtypeStruct(master.shape, jnp.bfloat16)]
    outs += [jax.ShapeDtypeStruct((SLOTS, CB, CB), jnp.bfloat16)] * 8
    vm = pl.BlockSpec(memory_space=pltpu.VMEM)
    return pl.pallas_call(
        tail_kernel,
        grid_spec=pltpu.PrefetchScalarGridSpec(
            num_scalar_prefetch=2,
            grid=(),
            in_specs=[vm] * 7,
            out_specs=[vm] * 12,
            scratch_shapes=[
                pltpu.VMEM((14 * CB, CB), jnp.float32),
                pltpu.VMEM((hot, CB), jnp.float32),
                pltpu.VMEM((8 * SLOTS, CB, CB), jnp.bfloat16),
            ],
        ),
        out_shape=outs,
        compiler_params=pltpu.CompilerParams(vmem_limit_bytes=24 * MiB),
        name="tail",
    )(ids, owners, *gs, master, moment, second)


def join_kernel(a_ref, b_ref, c_ref, d_ref, *refs):
    z_refs, o_ref, cold_ref, sem = refs[:8], refs[8], refs[9], refs[10]
    z = lax.axis_index("tensor")
    copies = [
        pltpu.make_async_copy(
            z_refs[d],
            cold_ref.at[pl.ds(((z - d) & 7) * SLOTS, SLOTS)],
            sem.at[d],
        )
        for d in range(8)
    ]
    for cp in copies:
        cp.start()
    for r, piece in enumerate(
        (a_ref[...], b_ref[...], c_ref[0], c_ref[1], d_ref[0], d_ref[1], d_ref[2], d_ref[3])
    ):
        o_ref[:, pl.ds(pl.multiple_of(pipe_block(r >> 1, r & 1) * CB, CB), CB)] = piece
    for cp in copies:
        cp.wait()


def joined(a, b, c, d, recv):
    return pl.pallas_call(
        join_kernel,
        in_specs=[VM] * 12,
        out_specs=[VM, HB],
        scratch_shapes=[pltpu.SemaphoreType.DMA((8,))],
        out_shape=[
            jax.ShapeDtypeStruct((a.shape[0], 8 * CB), a.dtype),
            jax.ShapeDtypeStruct((8 * SLOTS, CB, CB), jnp.bfloat16),
        ],
        compiler_params=pltpu.CompilerParams(vmem_limit_bytes=8 * MiB),
        name="join",
    )(a, b, c, d, *recv)


def wide(*xs):
    out = xs[0].astype(jnp.float32)
    for x in xs[1:]:
        out = out + x.astype(jnp.float32)
    return out


def shards(
    acts, grad_hidden, token_count, hot_ids, block_owner, master_hot, moment_hot, second_hot
):
    acts_v, *left = loaded(token_count, acts, grad_hidden)

    def mm(k, half, owns):
        return product(token_count, left[k], acts_v, k, half, owns)

    def moved(v, axis, pairs):
        return lax.ppermute(v, axis, pairs)

    def summed(*xs):
        return wide(*xs).astype(jnp.bfloat16)

    first = []
    for k in range(4):
        (peer,) = mm(k, 1, (0,))
        got = moved(peer, "pipe_1", SWAP)
        (mine,) = mm(k, 1, (1,))
        first.append(moved(summed(mine, got), *DIMS[k]))
    parts = []
    for k in range(4):
        peer, mine = mm(k, 0, (0, 1))
        parts.append([mine, moved(peer, "pipe_1", SWAP), first[k]])
    size = 8
    for s in range(1, 4):
        half = size // 2
        for k in range(4):
            send = summed(*[p[half:size] for p in parts[k]])
            parts[k].append(moved(send, *DIMS[(k + s) % 4]))
        size = half
    gs = []
    for k in range(4):
        gs.append(wide(*[p[0] for p in parts[k]]))
    outs = tail(hot_ids, block_owner[:, 0], gs, master_hot, moment_hot, second_hot)
    new_master, new_moment, new_second, hw = outs[:4]
    packs = outs[4:]
    recv = [packs[0]]
    for d in range(1, 8):
        recv.append(moved(packs[d], "tensor", [(i, (i + d) % 8) for i in range(8)]))
    hw_b = moved(hw, "pipe_1", SWAP)
    two = jnp.stack([hw, hw_b])
    hw_c = moved(two, "pipe_0", EVEN)
    hw_d = moved(jnp.concatenate([two, hw_c]), "pipe_0", ODD)
    hot_weights, cold = joined(hw, hw_b, hw_c, hw_d, recv)
    return (new_master, new_moment, new_second, hot_weights, cold)


def solution(mesh):
    split = Mesh(
        mesh.devices.reshape(mesh.shape["dp"], mesh.shape["tensor"], 4, 2),
        ("dp", "tensor", "pipe_0", "pipe_1"),
    )
    return jax.shard_map(
        shards,
        mesh=split,
        in_specs=(
            P(DP_PIPE, None),
            P(DP_PIPE, "tensor"),
            P(DP_PIPE),
            P("tensor", None),
            P("tensor", None),
            P("tensor", DP_PIPE),
            P("tensor", DP_PIPE),
            P("tensor", DP_PIPE),
        ),
        out_specs=(
            P("tensor", DP_PIPE),
            P("tensor", DP_PIPE),
            P("tensor", DP_PIPE),
            P("tensor", "dp"),
            P("tensor", DP_PIPE, None),
        ),
        check_vma=False,
    )
```

```python
import functools

import jax
import jax.numpy as jnp
from jax import lax
from jax.experimental import pallas as pl
from jax.experimental.pallas import tpu as pltpu
from jax.sharding import Mesh
from jax.sharding import PartitionSpec as P


CB = 128
DP_PIPE = ("dp", "pipe_0", "pipe_1")
SLOTS = 4
COLOURS = ((0, 4), (4, 4), (8, 3), (11, 3))
SPARE = 16
EVEN = [(0, 1), (1, 0), (2, 3), (3, 2)]
ODD = [(1, 2), (2, 1), (3, 0), (0, 3)]
DIMS = (("pipe_0", EVEN), ("dp", EVEN), ("pipe_0", ODD), ("dp", ODD))
SWAP = [(0, 1), (1, 0)]
ORDERS = ((0, 1, 2, 3), (1, 2, 3, 0), (2, 3, 0, 1), (3, 0, 1, 2))
MiB = 1 << 20


def gray(p):
    return p ^ (p >> 1)


def dest_block(k, half, own, q):
    idx = half * 8 + q
    rx = ry = 0
    for s in range(4):
        bit = (idx >> (3 - s)) & 1
        d = ORDERS[k][s]
        if d % 2 == 0:
            rx |= bit << (d // 2)
        else:
            ry |= bit << (d // 2)
    return far(lax.axis_index("dp"), ry) * 8 + pipe_block(rx, 1 - own)


def far(p, r):
    return gray(gray(p) ^ r)


def pipe_block(rx, rc):
    return far(lax.axis_index("pipe_0"), rx) * 2 + (lax.axis_index("pipe_1") ^ rc)


def load_kernel(cnt_ref, a_hbm, g_hbm, a_ref, l0, l1, l2, l3, stage, a_sem, g_sem):
    toks = stage.shape[1]
    g_copies = [
        pltpu.make_async_copy(
            g_hbm.at[:, first * CB : (first + n) * CB],
            stage.at[k, :, : n * CB],
            g_sem.at[k],
        )
        for k, (first, n) in enumerate(COLOURS)
    ]
    a_copy = pltpu.make_async_copy(a_hbm, a_ref, a_sem)
    for cp in g_copies:
        cp.start()
    a_copy.start()
    live = lax.broadcasted_iota(jnp.int32, (toks, CB), 0) < cnt_ref[0]
    for k, ((first, n), out) in enumerate(zip(COLOURS, (l0, l1, l2, l3))):
        g_copies[k].wait()
        for i in range(n):
            v = stage[k, :, i * CB : (i + 1) * CB]
            out[i * CB : (i + 1) * CB, :] = jnp.where(live, v, jnp.zeros_like(v)).T
    a_copy.wait()


VM = pl.BlockSpec(memory_space=pltpu.VMEM)
HB = pl.BlockSpec(memory_space=pltpu.HBM)


def loaded(cnt, acts, grad_hidden):
    toks = acts.shape[0]
    outs = [jax.ShapeDtypeStruct(acts.shape, acts.dtype)]
    outs += [jax.ShapeDtypeStruct((n * CB, toks), jnp.bfloat16) for _, n in COLOURS]
    return pl.pallas_call(
        load_kernel,
        grid_spec=pltpu.PrefetchScalarGridSpec(
            num_scalar_prefetch=1,
            grid=(),
            in_specs=[HB, HB],
            out_specs=[VM] * 5,
            scratch_shapes=[
                pltpu.VMEM((4, toks, 4 * CB), jnp.bfloat16),
                pltpu.SemaphoreType.DMA,
                pltpu.SemaphoreType.DMA((4,)),
            ],
        ),
        out_shape=outs,
        compiler_params=pltpu.CompilerParams(vmem_limit_bytes=16 * MiB),
        cost_estimate=pl.CostEstimate(flops=2000000000, bytes_accessed=0, transcendentals=0),
        name="load",
    )(
        cnt,
        pltpu.with_memory_space_constraint(acts, pltpu.HBM),
        pltpu.with_memory_space_constraint(grad_hidden, pltpu.HBM),
    )


def mm_kernel(cnt_ref, l_ref, a_ref, *outs, spare, k, half, owns):
    n = l_ref.shape[0]
    left = l_ref
    for o_ref, own in zip(outs, owns):

        def pair(i, _, o_ref=o_ref, own=own):
            blk = [
                a_ref[:, pl.ds(pl.multiple_of(dest_block(k, half, own, 2 * i + j) * CB, CB), CB)]
                for j in range(2)
            ]
            r = jnp.dot(
                left[...], jnp.concatenate(blk, axis=1), preferred_element_type=jnp.float32
            ).astype(jnp.bfloat16)
            o_ref[2 * i, :n, :] = r[:, :CB]
            o_ref[2 * i + 1, :n, :] = r[:, CB:]
            return 0

        lax.fori_loop(0, 4, pair, 0, unroll=4 if half else 2)
        if spare:
            c = cnt_ref[0]
            row = lax.broadcasted_iota(jnp.int32, (SPARE, CB), 0)
            digit = jnp.where(
                row == 0, c & 7, jnp.where(row == 1, (c >> 3) & 7, jnp.where(row == 2, c >> 6, 0))
            )
            digit = digit.astype(jnp.float32).astype(jnp.bfloat16)
            for i in range(8):
                o_ref[i, n:, :] = digit


def product(cnt, left, acts, k, half, owns):
    toks = acts.shape[0]
    n = left.shape[0]
    spare = SPARE if k == 3 else 0
    return pl.pallas_call(
        functools.partial(mm_kernel, spare=spare, k=k, half=half, owns=owns),
        grid_spec=pltpu.PrefetchScalarGridSpec(
            num_scalar_prefetch=1,
            grid=(),
            in_specs=[VM, VM],
            out_specs=[VM] * len(owns),
        ),
        out_shape=[jax.ShapeDtypeStruct((8, n + spare, CB), jnp.bfloat16)] * len(owns),
        compiler_params=pltpu.CompilerParams(vmem_limit_bytes=8 * MiB),
        cost_estimate=pl.CostEstimate(
            flops=2 * 8 * CB * n * toks * len(owns), bytes_accessed=0, transcendentals=0
        ),
        name="mm",
    )(cnt, left, acts)


PACKS = {d: ((d, 0, SLOTS),) for d in range(8)}


def tail_kernel(ids_ref, own_ref, g0, g1, g2, g3, hot_ref, *refs):
    z_refs, acc, pack = refs[:8], refs[8], refs[9]
    for (first, nblk), g in zip(COLOURS, (g0, g1, g2, g3)):
        acc[first * CB : (first + nblk) * CB, :] = g[: nblk * CB, :]
    digits = g3[COLOURS[3][1] * CB : COLOURS[3][1] * CB + 8, :]
    total = digits[0:1, :] + 8.0 * digits[1:2, :] + 64.0 * digits[2:3, :]
    pack[...] = jnp.zeros_like(pack)

    def take(i, _):
        h = ids_ref[0, i]
        hot_ref[pl.ds(i, 1), :] = acc[pl.ds(h, 1), :] / total
        acc[pl.ds(h, 1), :] = jnp.zeros((1, CB), jnp.float32)
        return 0

    lax.fori_loop(0, hot_ref.shape[0], take, 0, unroll=4)
    for b in range(acc.shape[0] // CB):
        x = acc[b * CB : (b + 1) * CB, :] / total
        owner = own_ref[b]
        slot = jnp.int32(0)
        for e in range(b):
            slot += (own_ref[e] == owner).astype(jnp.int32)
        pack[((owner - lax.axis_index("tensor")) & 7) * SLOTS + slot] = x.T.astype(jnp.bfloat16)
    for d in range(8):
        at = 0
        for e, lo, n in PACKS[d]:
            z_refs[d][at : at + n] = pack[e * SLOTS + lo : e * SLOTS + lo + n]
            at += n


def tail(ids, owners, gs, count):
    outs = [jax.ShapeDtypeStruct((count, CB), jnp.float32)]
    for d in range(8):
        outs.append(jax.ShapeDtypeStruct((sum(p[2] for p in PACKS[d]), CB, CB), jnp.bfloat16))
    return pl.pallas_call(
        tail_kernel,
        grid_spec=pltpu.PrefetchScalarGridSpec(
            num_scalar_prefetch=2,
            grid=(),
            in_specs=[VM] * 4,
            out_specs=[VM] * 9,
            scratch_shapes=[
                pltpu.VMEM((14 * CB, CB), jnp.float32),
                pltpu.VMEM((8 * SLOTS, CB, CB), jnp.bfloat16),
            ],
        ),
        out_shape=outs,
        compiler_params=pltpu.CompilerParams(vmem_limit_bytes=24 * MiB),
        name="tail",
    )(ids, owners, *gs)


def adam_kernel(g_ref, ma_ref, mo_ref, se_ref, nma_ref, nmo_ref, nse_ref, hw_ref):
    g_hot = g_ref[...]
    mo = 0.9 * mo_ref[...] + 0.1 * g_hot
    se = 0.95 * se_ref[...] + 0.05 * g_hot * g_hot
    bias_one = 1.0 - 0.9**4
    bias_two = 1.0 - 0.95**4
    ma = ma_ref[...] - 0.02 * (mo / bias_one) / (jnp.sqrt(se / bias_two) + 1e-08)
    nmo_ref[...] = mo
    nse_ref[...] = se
    nma_ref[...] = ma
    hw_ref[...] = ma.astype(jnp.bfloat16)


def adam(g_hot, master, moment, second):
    f32 = jax.ShapeDtypeStruct(master.shape, jnp.float32)
    return pl.pallas_call(
        adam_kernel,
        in_specs=[VM] * 4,
        out_specs=[VM] * 4,
        out_shape=[f32, f32, f32, jax.ShapeDtypeStruct(master.shape, jnp.bfloat16)],
        compiler_params=pltpu.CompilerParams(vmem_limit_bytes=8 * MiB),
        name="adam",
    )(g_hot, master, moment, second)


PLACES = tuple((d, 0, SLOTS) for d in range(8))


def join_kernel(a_ref, b_ref, c_ref, d_ref, *refs):
    z_refs, o_ref, cold_ref, sem = refs[:8], refs[8], refs[9], refs[10]
    z = lax.axis_index("tensor")
    copies = []
    for i, (d, lo, n) in enumerate(PLACES):
        at = ((z - d) & 7) * SLOTS + lo
        copies.append(
            pltpu.make_async_copy(z_refs[i].at[0:n], cold_ref.at[pl.ds(at, n)], sem.at[i])
        )
    for cp in copies:
        cp.start()
    for r, piece in enumerate(
        (a_ref[...], b_ref[...], c_ref[0], c_ref[1], d_ref[0], d_ref[1], d_ref[2], d_ref[3])
    ):
        o_ref[:, pl.ds(pl.multiple_of(pipe_block(r >> 1, r & 1) * CB, CB), CB)] = piece
    for cp in copies:
        cp.wait()


def joined(a, b, c, d, recv):
    return pl.pallas_call(
        join_kernel,
        in_specs=[VM] * 12,
        out_specs=[VM, HB],
        scratch_shapes=[pltpu.SemaphoreType.DMA((8,))],
        out_shape=[
            jax.ShapeDtypeStruct((a.shape[0], 8 * CB), a.dtype),
            jax.ShapeDtypeStruct((8 * SLOTS, CB, CB), jnp.bfloat16),
        ],
        compiler_params=pltpu.CompilerParams(vmem_limit_bytes=8 * MiB),
        name="join",
    )(a, b, c, d, *recv)


def wide(*xs):
    out = xs[0].astype(jnp.float32)
    for x in xs[1:]:
        out = out + x.astype(jnp.float32)
    return out


def shards(
    acts, grad_hidden, token_count, hot_ids, block_owner, master_hot, moment_hot, second_hot
):
    acts_v, *left = loaded(token_count, acts, grad_hidden)

    def mm(k, half, owns):
        return product(token_count, left[k], acts_v, k, half, owns)

    def moved(v, axis, pairs):
        return lax.ppermute(v, axis, pairs)

    def summed(*xs):
        return wide(*xs).astype(jnp.bfloat16)

    first = []
    for k in range(4):
        (peer,) = mm(k, 1, (0,))
        got = moved(peer, "pipe_1", SWAP)
        (mine,) = mm(k, 1, (1,))
        first.append(moved(summed(mine, got), *DIMS[ORDERS[k][0]]))
    parts = []
    for k in range(4):
        peer, mine = mm(k, 0, (0, 1))
        parts.append([mine, moved(peer, "pipe_1", SWAP), first[k]])
    size = 8
    for s in range(1, 4):
        half = size // 2
        for k in range(4):
            send = summed(*[p[half:size] for p in parts[k]])
            parts[k].append(moved(send, *DIMS[ORDERS[k][s]]))
        size = half
    gs = []
    for k in range(4):
        gs.append(wide(*[p[0] for p in parts[k]]))
    g_hot, *packs = tail(hot_ids, block_owner[:, 0], gs, hot_ids.shape[1])
    new_master, new_moment, new_second, hw = adam(g_hot, master_hot, moment_hot, second_hot)
    recv = [packs[0]]
    for d in range(1, 8):
        recv.append(moved(packs[d], "tensor", [(i, (i + d) % 8) for i in range(8)]))
    hw_b = moved(hw, "pipe_1", SWAP)
    two = jnp.stack([hw, hw_b])
    hw_c = moved(two, "pipe_0", EVEN)
    hw_d = moved(jnp.concatenate([two, hw_c]), "pipe_0", ODD)
    hot_weights, cold = joined(hw, hw_b, hw_c, hw_d, recv)
    return (new_master, new_moment, new_second, hot_weights, cold)


def solution(mesh):
    split = Mesh(
        mesh.devices.reshape(mesh.shape["dp"], mesh.shape["tensor"], 4, 2),
        ("dp", "tensor", "pipe_0", "pipe_1"),
    )
    return jax.shard_map(
        shards,
        mesh=split,
        in_specs=(
            P(DP_PIPE, None),
            P(DP_PIPE, "tensor"),
            P(DP_PIPE),
            P("tensor", None),
            P("tensor", None),
            P("tensor", DP_PIPE),
            P("tensor", DP_PIPE),
            P("tensor", DP_PIPE),
        ),
        out_specs=(
            P("tensor", DP_PIPE),
            P("tensor", DP_PIPE),
            P("tensor", DP_PIPE),
            P("tensor", "dp"),
            P("tensor", DP_PIPE, None),
        ),
        check_vma=False,
    )
```

```python
import functools

import jax
import jax.numpy as jnp
from jax import lax
from jax.experimental import pallas as pl
from jax.experimental.pallas import tpu as pltpu
from jax.sharding import Mesh
from jax.sharding import PartitionSpec as P


CB = 128
DP_PIPE = ("dp", "pipe_0", "pipe_1")
SLOTS = 4
COLOURS = ((0, 4), (4, 4), (8, 3), (11, 3))
SPARE = 16
EVEN = [(0, 1), (1, 0), (2, 3), (3, 2)]
ODD = [(1, 2), (2, 1), (3, 0), (0, 3)]
DIMS = (("pipe_0", EVEN), ("dp", EVEN), ("pipe_0", ODD), ("dp", ODD))
SWAP = [(0, 1), (1, 0)]
ORDERS = ((0, 1, 3, 2), (1, 0, 2, 3), (2, 3, 0, 1), (3, 2, 1, 0))
MiB = 1 << 20


def gray(p):
    return p ^ (p >> 1)


def dest_block(k, half, own, q):
    idx = half * 8 + q
    rx = ry = 0
    for s in range(4):
        bit = (idx >> (3 - s)) & 1
        d = ORDERS[k][s]
        if d % 2 == 0:
            rx |= bit << (d // 2)
        else:
            ry |= bit << (d // 2)
    return far(lax.axis_index("dp"), ry) * 8 + pipe_block(rx, 1 - own)


def far(p, r):
    return gray(gray(p) ^ r)


def pipe_block(rx, rc):
    return far(lax.axis_index("pipe_0"), rx) * 2 + (lax.axis_index("pipe_1") ^ rc)


def load_kernel(cnt_ref, a_hbm, g_hbm, a_ref, l0, l1, l2, l3, stage, a_sem, g_sem):
    toks = stage.shape[1]
    g_copies = [
        pltpu.make_async_copy(
            g_hbm.at[:, first * CB : (first + n) * CB],
            stage.at[k, :, : n * CB],
            g_sem.at[k],
        )
        for k, (first, n) in enumerate(COLOURS)
    ]
    a_copy = pltpu.make_async_copy(a_hbm, a_ref, a_sem)
    for cp in g_copies:
        cp.start()
    a_copy.start()
    live = lax.broadcasted_iota(jnp.int32, (toks, CB), 0) < cnt_ref[0]
    for k, ((first, n), out) in enumerate(zip(COLOURS, (l0, l1, l2, l3))):
        g_copies[k].wait()
        for i in range(n):
            v = stage[k, :, i * CB : (i + 1) * CB]
            out[i * CB : (i + 1) * CB, :] = jnp.where(live, v, jnp.zeros_like(v)).T
    a_copy.wait()


VM = pl.BlockSpec(memory_space=pltpu.VMEM)
HB = pl.BlockSpec(memory_space=pltpu.HBM)


def loaded(cnt, acts, grad_hidden):
    toks = acts.shape[0]
    outs = [jax.ShapeDtypeStruct(acts.shape, acts.dtype)]
    outs += [jax.ShapeDtypeStruct((n * CB, toks), jnp.bfloat16) for _, n in COLOURS]
    return pl.pallas_call(
        load_kernel,
        grid_spec=pltpu.PrefetchScalarGridSpec(
            num_scalar_prefetch=1,
            grid=(),
            in_specs=[HB, HB],
            out_specs=[VM] * 5,
            scratch_shapes=[
                pltpu.VMEM((4, toks, 4 * CB), jnp.bfloat16),
                pltpu.SemaphoreType.DMA,
                pltpu.SemaphoreType.DMA((4,)),
            ],
        ),
        out_shape=outs,
        compiler_params=pltpu.CompilerParams(vmem_limit_bytes=16 * MiB),
        cost_estimate=pl.CostEstimate(flops=2000000000, bytes_accessed=0, transcendentals=0),
        name="load",
    )(
        cnt,
        pltpu.with_memory_space_constraint(acts, pltpu.HBM),
        pltpu.with_memory_space_constraint(grad_hidden, pltpu.HBM),
    )


def mm_kernel(cnt_ref, l_ref, a_ref, *outs, spare, k, half, owns):
    n = l_ref.shape[0]
    left = l_ref
    for o_ref, own in zip(outs, owns):

        def pair(i, _, o_ref=o_ref, own=own):
            blk = [
                a_ref[:, pl.ds(pl.multiple_of(dest_block(k, half, own, 2 * i + j) * CB, CB), CB)]
                for j in range(2)
            ]
            r = jnp.dot(
                left[...], jnp.concatenate(blk, axis=1), preferred_element_type=jnp.float32
            ).astype(jnp.bfloat16)
            o_ref[2 * i, :n, :] = r[:, :CB]
            o_ref[2 * i + 1, :n, :] = r[:, CB:]
            return 0

        lax.fori_loop(0, 4, pair, 0, unroll=4 if half else 2)
        if spare:
            c = cnt_ref[0]
            row = lax.broadcasted_iota(jnp.int32, (SPARE, CB), 0)
            digit = jnp.where(
                row == 0, c & 7, jnp.where(row == 1, (c >> 3) & 7, jnp.where(row == 2, c >> 6, 0))
            )
            digit = digit.astype(jnp.float32).astype(jnp.bfloat16)
            for i in range(8):
                o_ref[i, n:, :] = digit


def product(cnt, left, acts, k, half, owns):
    toks = acts.shape[0]
    n = left.shape[0]
    spare = SPARE if k == 3 else 0
    return pl.pallas_call(
        functools.partial(mm_kernel, spare=spare, k=k, half=half, owns=owns),
        grid_spec=pltpu.PrefetchScalarGridSpec(
            num_scalar_prefetch=1,
            grid=(),
            in_specs=[VM, VM],
            out_specs=[VM] * len(owns),
        ),
        out_shape=[jax.ShapeDtypeStruct((8, n + spare, CB), jnp.bfloat16)] * len(owns),
        compiler_params=pltpu.CompilerParams(vmem_limit_bytes=8 * MiB),
        cost_estimate=pl.CostEstimate(
            flops=2 * 8 * CB * n * toks * len(owns), bytes_accessed=0, transcendentals=0
        ),
        name="mm",
    )(cnt, left, acts)


PACKS = {d: ((d, 0, SLOTS),) for d in range(8)}


def tail_kernel(ids_ref, own_ref, g0, g1, g2, g3, hot_ref, *refs):
    z_refs, acc, pack = refs[:8], refs[8], refs[9]
    for (first, nblk), g in zip(COLOURS, (g0, g1, g2, g3)):
        acc[first * CB : (first + nblk) * CB, :] = g[: nblk * CB, :]
    digits = g3[COLOURS[3][1] * CB : COLOURS[3][1] * CB + 8, :]
    scale = 1.0 / (digits[0:1, :] + 8.0 * digits[1:2, :] + 64.0 * digits[2:3, :])
    pack[...] = jnp.zeros_like(pack)

    def take(i, _):
        h = ids_ref[0, i]
        hot_ref[pl.ds(i, 1), :] = acc[pl.ds(h, 1), :] * scale
        acc[pl.ds(h, 1), :] = jnp.zeros((1, CB), jnp.float32)
        return 0

    lax.fori_loop(0, hot_ref.shape[0], take, 0, unroll=4)
    for b in range(acc.shape[0] // CB):
        x = acc[b * CB : (b + 1) * CB, :] * scale
        owner = own_ref[b]
        slot = jnp.int32(0)
        for e in range(b):
            slot += (own_ref[e] == owner).astype(jnp.int32)
        pack[((owner - lax.axis_index("tensor")) & 7) * SLOTS + slot] = x.T.astype(jnp.bfloat16)
    for d in range(8):
        at = 0
        for e, lo, n in PACKS[d]:
            z_refs[d][at : at + n] = pack[e * SLOTS + lo : e * SLOTS + lo + n]
            at += n


def tail(ids, owners, gs, count):
    outs = [jax.ShapeDtypeStruct((count, CB), jnp.float32)]
    for d in range(8):
        outs.append(jax.ShapeDtypeStruct((sum(p[2] for p in PACKS[d]), CB, CB), jnp.bfloat16))
    return pl.pallas_call(
        tail_kernel,
        grid_spec=pltpu.PrefetchScalarGridSpec(
            num_scalar_prefetch=2,
            grid=(),
            in_specs=[VM] * 4,
            out_specs=[VM] * 9,
            scratch_shapes=[
                pltpu.VMEM((14 * CB, CB), jnp.float32),
                pltpu.VMEM((8 * SLOTS, CB, CB), jnp.bfloat16),
            ],
        ),
        out_shape=outs,
        compiler_params=pltpu.CompilerParams(vmem_limit_bytes=24 * MiB),
        name="tail",
    )(ids, owners, *gs)


def adam_kernel(g_ref, ma_ref, mo_ref, se_ref, nma_ref, nmo_ref, nse_ref, hw_ref):
    g_hot = g_ref[...]
    mo = 0.9 * mo_ref[...] + 0.1 * g_hot
    se = 0.95 * se_ref[...] + 0.05 * g_hot * g_hot
    bias_one = 1.0 - 0.9**4
    bias_two = 1.0 - 0.95**4
    ma = ma_ref[...] - 0.02 * (mo / bias_one) / (jnp.sqrt(se / bias_two) + 1e-08)
    nmo_ref[...] = mo
    nse_ref[...] = se
    nma_ref[...] = ma
    hw_ref[...] = ma.astype(jnp.bfloat16)


def adam(g_hot, master, moment, second):
    f32 = jax.ShapeDtypeStruct(master.shape, jnp.float32)
    return pl.pallas_call(
        adam_kernel,
        in_specs=[VM] * 4,
        out_specs=[VM] * 4,
        out_shape=[f32, f32, f32, jax.ShapeDtypeStruct(master.shape, jnp.bfloat16)],
        compiler_params=pltpu.CompilerParams(vmem_limit_bytes=8 * MiB),
        name="adam",
    )(g_hot, master, moment, second)


PLACES = tuple((d, 0, SLOTS) for d in range(8))


def join_kernel(a_ref, b_ref, c_ref, d_ref, *refs):
    z_refs, o_ref, cold_ref, sem = refs[:8], refs[8], refs[9], refs[10]
    z = lax.axis_index("tensor")
    copies = []
    for i, (d, lo, n) in enumerate(PLACES):
        at = ((z - d) & 7) * SLOTS + lo
        copies.append(
            pltpu.make_async_copy(z_refs[i].at[0:n], cold_ref.at[pl.ds(at, n)], sem.at[i])
        )
    for cp in copies:
        cp.start()
    for r, piece in enumerate(
        (a_ref[...], b_ref[...], c_ref[0], c_ref[1], d_ref[0], d_ref[1], d_ref[2], d_ref[3])
    ):
        o_ref[:, pl.ds(pl.multiple_of(pipe_block(r >> 1, r & 1) * CB, CB), CB)] = piece
    for cp in copies:
        cp.wait()


def joined(a, b, c, d, recv):
    return pl.pallas_call(
        join_kernel,
        in_specs=[VM] * 12,
        out_specs=[VM, HB],
        scratch_shapes=[pltpu.SemaphoreType.DMA((8,))],
        out_shape=[
            jax.ShapeDtypeStruct((a.shape[0], 8 * CB), a.dtype),
            jax.ShapeDtypeStruct((8 * SLOTS, CB, CB), jnp.bfloat16),
        ],
        compiler_params=pltpu.CompilerParams(vmem_limit_bytes=8 * MiB),
        name="join",
    )(a, b, c, d, *recv)


def wide(*xs):
    out = xs[0].astype(jnp.float32)
    for x in xs[1:]:
        out = out + x.astype(jnp.float32)
    return out


def shards(
    acts, grad_hidden, token_count, hot_ids, block_owner, master_hot, moment_hot, second_hot
):
    acts_v, *left = loaded(token_count, acts, grad_hidden)

    def mm(k, half, owns):
        return product(token_count, left[k], acts_v, k, half, owns)

    def moved(v, axis, pairs):
        return lax.ppermute(v, axis, pairs)

    def summed(*xs):
        return wide(*xs).astype(jnp.bfloat16)

    first = []
    for k in range(4):
        (peer,) = mm(k, 1, (0,))
        got = moved(peer, "pipe_1", SWAP)
        (mine,) = mm(k, 1, (1,))
        first.append(moved(summed(mine, got), *DIMS[ORDERS[k][0]]))
    parts = []
    for k in range(4):
        peer, mine = mm(k, 0, (0, 1))
        parts.append([mine, moved(peer, "pipe_1", SWAP), first[k]])
    size = 8
    for s in range(1, 4):
        half = size // 2
        for k in range(4):
            send = summed(*[p[half:size] for p in parts[k]])
            parts[k].append(moved(send, *DIMS[ORDERS[k][s]]))
        size = half
    gs = []
    for k in range(4):
        gs.append(wide(*[p[0] for p in parts[k]]))
    g_hot, *packs = tail(hot_ids, block_owner[:, 0], gs, hot_ids.shape[1])
    new_master, new_moment, new_second, hw = adam(g_hot, master_hot, moment_hot, second_hot)
    recv = [packs[0]]
    for d in range(1, 8):
        recv.append(moved(packs[d], "tensor", [(i, (i + d) % 8) for i in range(8)]))
    hw_b = moved(hw, "pipe_1", SWAP)
    two = jnp.stack([hw, hw_b])
    hw_c = moved(two, "pipe_0", EVEN)
    hw_d = moved(jnp.concatenate([two, hw_c]), "pipe_0", ODD)
    hot_weights, cold = joined(hw, hw_b, hw_c, hw_d, recv)
    return (new_master, new_moment, new_second, hot_weights, cold)


def solution(mesh):
    split = Mesh(
        mesh.devices.reshape(mesh.shape["dp"], mesh.shape["tensor"], 4, 2),
        ("dp", "tensor", "pipe_0", "pipe_1"),
    )
    return jax.shard_map(
        shards,
        mesh=split,
        in_specs=(
            P(DP_PIPE, None),
            P(DP_PIPE, "tensor"),
            P(DP_PIPE),
            P("tensor", None),
            P("tensor", None),
            P("tensor", DP_PIPE),
            P("tensor", DP_PIPE),
            P("tensor", DP_PIPE),
        ),
        out_specs=(
            P("tensor", DP_PIPE),
            P("tensor", DP_PIPE),
            P("tensor", DP_PIPE),
            P("tensor", "dp"),
            P("tensor", DP_PIPE, None),
        ),
        check_vma=False,
    )
```

```python
import functools

import jax
import jax.numpy as jnp
from jax import lax
from jax.experimental import pallas as pl
from jax.experimental.pallas import tpu as pltpu
from jax.sharding import Mesh
from jax.sharding import PartitionSpec as P


CB = 128
DP_PIPE = ("dp", "pipe_0", "pipe_1")
SLOTS = 4
COLOURS = ((0, 4), (4, 4), (8, 3), (11, 3))
SPARE = 16
EVEN = [(0, 1), (1, 0), (2, 3), (3, 2)]
ODD = [(1, 2), (2, 1), (3, 0), (0, 3)]
DIMS = (("pipe_0", EVEN), ("dp", EVEN), ("pipe_0", ODD), ("dp", ODD))
SWAP = [(0, 1), (1, 0)]
ORDERS = ((0, 1, 3, 2), (1, 0, 2, 3), (2, 3, 0, 1), (3, 2, 1, 0))
MiB = 1 << 20


def gray(p):
    return p ^ (p >> 1)


def dest_block(k, half, own, q):
    idx = half * 8 + q
    rx = ry = 0
    for s in range(4):
        bit = (idx >> (3 - s)) & 1
        d = ORDERS[k][s]
        if d % 2 == 0:
            rx |= bit << (d // 2)
        else:
            ry |= bit << (d // 2)
    return far(lax.axis_index("dp"), ry) * 8 + pipe_block(rx, 1 - own)


def far(p, r):
    return gray(gray(p) ^ r)


def pipe_block(rx, rc):
    return far(lax.axis_index("pipe_0"), rx) * 2 + (lax.axis_index("pipe_1") ^ rc)


def load_kernel(cnt_ref, a_hbm, g_hbm, a_ref, l0, l1, l2, l3, stage, a_sem, g_sem):
    toks = stage.shape[1]
    g_copies = [
        pltpu.make_async_copy(
            g_hbm.at[:, first * CB : (first + n) * CB],
            stage.at[k, :, : n * CB],
            g_sem.at[k],
        )
        for k, (first, n) in enumerate(COLOURS)
    ]
    a_copy = pltpu.make_async_copy(a_hbm, a_ref, a_sem)
    for cp in g_copies:
        cp.start()
    a_copy.start()
    live = lax.broadcasted_iota(jnp.int32, (toks, CB), 0) < cnt_ref[0]
    for k, ((first, n), out) in enumerate(zip(COLOURS, (l0, l1, l2, l3))):
        g_copies[k].wait()
        for i in range(n):
            v = stage[k, :, i * CB : (i + 1) * CB]
            out[i * CB : (i + 1) * CB, :] = jnp.where(live, v, jnp.zeros_like(v)).T
    a_copy.wait()


VM = pl.BlockSpec(memory_space=pltpu.VMEM)
HB = pl.BlockSpec(memory_space=pltpu.HBM)


def loaded(cnt, acts, grad_hidden):
    toks = acts.shape[0]
    outs = [jax.ShapeDtypeStruct(acts.shape, acts.dtype)]
    outs += [jax.ShapeDtypeStruct((n * CB, toks), jnp.bfloat16) for _, n in COLOURS]
    return pl.pallas_call(
        load_kernel,
        grid_spec=pltpu.PrefetchScalarGridSpec(
            num_scalar_prefetch=1,
            grid=(),
            in_specs=[HB, HB],
            out_specs=[VM] * 5,
            scratch_shapes=[
                pltpu.VMEM((4, toks, 4 * CB), jnp.bfloat16),
                pltpu.SemaphoreType.DMA,
                pltpu.SemaphoreType.DMA((4,)),
            ],
        ),
        out_shape=outs,
        compiler_params=pltpu.CompilerParams(vmem_limit_bytes=16 * MiB),
        cost_estimate=pl.CostEstimate(flops=2000000000, bytes_accessed=0, transcendentals=0),
        name="load",
    )(
        cnt,
        pltpu.with_memory_space_constraint(acts, pltpu.HBM),
        pltpu.with_memory_space_constraint(grad_hidden, pltpu.HBM),
    )


def mm_kernel(cnt_ref, l_ref, a_ref, *outs, spare, k, half, owns):
    n = l_ref.shape[0]
    left = l_ref
    for o_ref, own in zip(outs, owns):

        def pair(i, _, o_ref=o_ref, own=own):
            blk = [
                a_ref[:, pl.ds(pl.multiple_of(dest_block(k, half, own, 2 * i + j) * CB, CB), CB)]
                for j in range(2)
            ]
            r = jnp.dot(
                left[...], jnp.concatenate(blk, axis=1), preferred_element_type=jnp.float32
            ).astype(jnp.bfloat16)
            o_ref[2 * i, :n, :] = r[:, :CB]
            o_ref[2 * i + 1, :n, :] = r[:, CB:]
            return 0

        lax.fori_loop(0, 4, pair, 0, unroll=4 if half else 2)
        if spare:
            c = cnt_ref[0]
            row = lax.broadcasted_iota(jnp.int32, (SPARE, CB), 0)
            digit = jnp.where(
                row == 0, c & 7, jnp.where(row == 1, (c >> 3) & 7, jnp.where(row == 2, c >> 6, 0))
            )
            digit = digit.astype(jnp.float32).astype(jnp.bfloat16)
            for i in range(8):
                o_ref[i, n:, :] = digit


def product(cnt, left, acts, k, half, owns):
    toks = acts.shape[0]
    n = left.shape[0]
    spare = SPARE if k == 3 else 0
    return pl.pallas_call(
        functools.partial(mm_kernel, spare=spare, k=k, half=half, owns=owns),
        grid_spec=pltpu.PrefetchScalarGridSpec(
            num_scalar_prefetch=1,
            grid=(),
            in_specs=[VM, VM],
            out_specs=[VM] * len(owns),
        ),
        out_shape=[jax.ShapeDtypeStruct((8, n + spare, CB), jnp.bfloat16)] * len(owns),
        compiler_params=pltpu.CompilerParams(vmem_limit_bytes=8 * MiB),
        cost_estimate=pl.CostEstimate(
            flops=2 * 8 * CB * n * toks * len(owns), bytes_accessed=0, transcendentals=0
        ),
        name="mm",
    )(cnt, left, acts)


PACKS = {d: ((d, 0, SLOTS),) for d in range(8)}


def tail_kernel(ids_ref, own_ref, g0, g1, g2, g3, hot_ref, *refs):
    z_refs, acc, pack = refs[:8], refs[8], refs[9]
    for (first, nblk), g in zip(COLOURS, (g0, g1, g2, g3)):
        acc[first * CB : (first + nblk) * CB, :] = g[: nblk * CB, :]
    digits = g3[COLOURS[3][1] * CB : COLOURS[3][1] * CB + 8, :]
    scale = 1.0 / (digits[0:1, :] + 8.0 * digits[1:2, :] + 64.0 * digits[2:3, :])
    pack[...] = jnp.zeros_like(pack)

    def take(i, _):
        hot_ref[pl.ds(i, 1), :] = acc[pl.ds(ids_ref[0, i], 1), :] * scale
        return 0

    def clear(i, _):
        acc[pl.ds(ids_ref[0, i], 1), :] = jnp.zeros((1, CB), jnp.float32)
        return 0

    lax.fori_loop(0, hot_ref.shape[0], take, 0, unroll=16)
    lax.fori_loop(0, hot_ref.shape[0], clear, 0, unroll=16)
    for b in range(acc.shape[0] // CB):
        x = acc[b * CB : (b + 1) * CB, :] * scale
        owner = own_ref[b]
        slot = jnp.int32(0)
        for e in range(b):
            slot += (own_ref[e] == owner).astype(jnp.int32)
        pack[((owner - lax.axis_index("tensor")) & 7) * SLOTS + slot] = x.astype(jnp.bfloat16).T
    for d in range(8):
        at = 0
        for e, lo, n in PACKS[d]:
            z_refs[d][at : at + n] = pack[e * SLOTS + lo : e * SLOTS + lo + n]
            at += n


def tail(ids, owners, gs, count):
    outs = [jax.ShapeDtypeStruct((count, CB), jnp.float32)]
    for d in range(8):
        outs.append(jax.ShapeDtypeStruct((sum(p[2] for p in PACKS[d]), CB, CB), jnp.bfloat16))
    return pl.pallas_call(
        tail_kernel,
        grid_spec=pltpu.PrefetchScalarGridSpec(
            num_scalar_prefetch=2,
            grid=(),
            in_specs=[VM] * 4,
            out_specs=[VM] * 9,
            scratch_shapes=[
                pltpu.VMEM((14 * CB, CB), jnp.float32),
                pltpu.VMEM((8 * SLOTS, CB, CB), jnp.bfloat16),
            ],
        ),
        out_shape=outs,
        compiler_params=pltpu.CompilerParams(vmem_limit_bytes=24 * MiB),
        name="tail",
    )(ids, owners, *gs)


def adam_kernel(g_ref, ma_ref, mo_ref, se_ref, nma_ref, nmo_ref, nse_ref, hw_ref):
    g_hot = g_ref[...]
    mo = 0.9 * mo_ref[...] + 0.1 * g_hot
    se = 0.95 * se_ref[...] + 0.05 * g_hot * g_hot
    bias_one = 1.0 - 0.9**4
    bias_two = 1.0 - 0.95**4
    ma = ma_ref[...] - 0.02 * (mo / bias_one) / (jnp.sqrt(se / bias_two) + 1e-08)
    nmo_ref[...] = mo
    nse_ref[...] = se
    nma_ref[...] = ma
    hw_ref[...] = ma.astype(jnp.bfloat16)


def adam(g_hot, master, moment, second):
    f32 = jax.ShapeDtypeStruct(master.shape, jnp.float32)
    return pl.pallas_call(
        adam_kernel,
        in_specs=[VM] * 4,
        out_specs=[VM] * 4,
        out_shape=[f32, f32, f32, jax.ShapeDtypeStruct(master.shape, jnp.bfloat16)],
        compiler_params=pltpu.CompilerParams(vmem_limit_bytes=8 * MiB),
        name="adam",
    )(g_hot, master, moment, second)


PLACES = tuple((d, 0, SLOTS) for d in range(8))


def join_kernel(a_ref, b_ref, c_ref, d_ref, *refs):
    z_refs, o_ref, cold_ref, sem = refs[:8], refs[8], refs[9], refs[10]
    z = lax.axis_index("tensor")
    copies = []
    for i, (d, lo, n) in enumerate(PLACES):
        at = ((z - d) & 7) * SLOTS + lo
        copies.append(
            pltpu.make_async_copy(z_refs[i].at[0:n], cold_ref.at[pl.ds(at, n)], sem.at[i])
        )
    for cp in copies:
        cp.start()
    for r, piece in enumerate(
        (a_ref[...], b_ref[...], c_ref[0], c_ref[1], d_ref[0], d_ref[1], d_ref[2], d_ref[3])
    ):
        o_ref[:, pl.ds(pl.multiple_of(pipe_block(r >> 1, r & 1) * CB, CB), CB)] = piece
    for cp in copies:
        cp.wait()


def joined(a, b, c, d, recv):
    return pl.pallas_call(
        join_kernel,
        in_specs=[VM] * 12,
        out_specs=[VM, HB],
        scratch_shapes=[pltpu.SemaphoreType.DMA((8,))],
        out_shape=[
            jax.ShapeDtypeStruct((a.shape[0], 8 * CB), a.dtype),
            jax.ShapeDtypeStruct((8 * SLOTS, CB, CB), jnp.bfloat16),
        ],
        compiler_params=pltpu.CompilerParams(vmem_limit_bytes=8 * MiB),
        name="join",
    )(a, b, c, d, *recv)


def wide(*xs):
    out = xs[0].astype(jnp.float32)
    for x in xs[1:]:
        out = out + x.astype(jnp.float32)
    return out


def shards(
    acts, grad_hidden, token_count, hot_ids, block_owner, master_hot, moment_hot, second_hot
):
    acts_v, *left = loaded(token_count, acts, grad_hidden)

    def mm(k, half, owns):
        return product(token_count, left[k], acts_v, k, half, owns)

    def moved(v, axis, pairs):
        return lax.ppermute(v, axis, pairs)

    def summed(*xs):
        return wide(*xs).astype(jnp.bfloat16)

    first = []
    for k in range(4):
        (peer,) = mm(k, 1, (0,))
        got = moved(peer, "pipe_1", SWAP)
        (mine,) = mm(k, 1, (1,))
        first.append(moved(summed(mine, got), *DIMS[ORDERS[k][0]]))
    parts = []
    for k in range(4):
        peer, mine = mm(k, 0, (0, 1))
        parts.append([mine, moved(peer, "pipe_1", SWAP), first[k]])
    size = 8
    for s in range(1, 4):
        half = size // 2
        for k in range(4):
            send = summed(*[p[half:size] for p in parts[k]])
            parts[k].append(moved(send, *DIMS[ORDERS[k][s]]))
        size = half
    gs = []
    for k in range(4):
        gs.append(wide(*[p[0] for p in parts[k]]))
    g_hot, *packs = tail(hot_ids, block_owner[:, 0], gs, hot_ids.shape[1])
    new_master, new_moment, new_second, hw = adam(g_hot, master_hot, moment_hot, second_hot)
    recv = [packs[0]]
    for d in range(1, 8):
        recv.append(moved(packs[d], "tensor", [(i, (i + d) % 8) for i in range(8)]))
    hw_b = moved(hw, "pipe_1", SWAP)
    two = jnp.stack([hw, hw_b])
    hw_c = moved(two, "pipe_0", EVEN)
    hw_d = moved(jnp.concatenate([two, hw_c]), "pipe_0", ODD)
    hot_weights, cold = joined(hw, hw_b, hw_c, hw_d, recv)
    return (new_master, new_moment, new_second, hot_weights, cold)


def solution(mesh):
    split = Mesh(
        mesh.devices.reshape(mesh.shape["dp"], mesh.shape["tensor"], 4, 2),
        ("dp", "tensor", "pipe_0", "pipe_1"),
    )
    return jax.shard_map(
        shards,
        mesh=split,
        in_specs=(
            P(DP_PIPE, None),
            P(DP_PIPE, "tensor"),
            P(DP_PIPE),
            P("tensor", None),
            P("tensor", None),
            P("tensor", DP_PIPE),
            P("tensor", DP_PIPE),
            P("tensor", DP_PIPE),
        ),
        out_specs=(
            P("tensor", DP_PIPE),
            P("tensor", DP_PIPE),
            P("tensor", DP_PIPE),
            P("tensor", "dp"),
            P("tensor", DP_PIPE, None),
        ),
        check_vma=False,
    )
```
